32 devices in a mesh: grp: 2 (over y), hist: 4 (over z), chan: 2 (over x), seq: 2 (over core).
Axes of the slice: x: 2, y: 2, z: 4, core: 2. Of those that a mesh axis runs over, the one named last changes fastest.
Arguments:
- history: bfloat16 [16, 2048, 4096], P(('grp', 'seq'), 'hist', 'chan'), parts along dimension 0, may hold values from -6 to 6
- filter_taps: bfloat16 [4096, 4096], P(('grp', 'hist'), 'chan'), parts along dimension 0, may hold values from -0.125 to 0.125
- skip_gain: float32 [8192], P(('grp', 'chan')), parts along dimension 0, may hold values from -4 to 4
- gate_values: bfloat16 [16, 64, 4096], P(('grp', 'seq'), 'hist', 'chan'), parts along dimension 0, may hold values from -6 to 6
Outputs:
- output: bfloat16 [16, 64, 4096], P(('grp', 'seq'), 'hist', 'chan'), parts along dimension 0
The draws below stay inside these ranges and needn't reach their ends.
There are 2 independent parts, one for each index of `grp`. The reference program is written for one: setup_inputs(seed, part) draws one part's arguments, and reference() takes and returns one part's arrays. A program takes and returns all parts, laid end to end along the dimension named above; each array names one. Nothing has to cross between parts.
All inputs are finite; a program needn't handle non-finite values.
Results may differ from the reference program's by a relative error of at most 0.0085.
Values may be sent and summed in bfloat16 or wider, within the bound.
A program may use at most 192 MiB of HBM per device.

```python
import jax
import jax.numpy as jnp
from jax import lax

CH = 4096
SEQS = 8
NEW = 64
TOTAL = 2048


def steps_of(rng, dims, pieces, smallest, top_value):
    def one(axis_at, parts):
        steps = jax.random.uniform(jax.random.fold_in(jax.random.fold_in(rng, 6), axis_at), (parts,), jnp.float32, smallest / len(pieces), top_value / len(pieces))
        return jnp.repeat(jnp.exp(steps), dims[axis_at] // parts).reshape((-1,) + (1,) * (len(dims) - axis_at - 1))

    level = one(*pieces[0])
    for cut in pieces[1:]:
        level = level * one(*cut)
    return level


def scatter_about(rng, shape, spread, reach, pieces=(), dtype=jnp.bfloat16):
    loudness = steps_of(rng, shape, pieces, -0.22, 0.18) if pieces else 1.0
    values = jax.random.normal(rng, shape, jnp.float32) * spread * loudness
    return jnp.minimum(jnp.maximum(values, -reach), reach).astype(dtype)


def setup_inputs(seed: int = 0, part: int = 0) -> dict:
    arg_keys = jax.random.split(jax.random.key(seed), 5)
    part_keys = jax.random.split(jax.random.fold_in(arg_keys[4], part), 5)
    return {
        "history": scatter_about(part_keys[0], (SEQS, TOTAL, CH), 1.0, 6.0, ((0, 2), (1, 4), (2, 2))),
        "filter_taps": scatter_about(part_keys[1], (TOTAL, CH), TOTAL ** -0.5, 0.125, ((0, 4), (1, 2))),
        "skip_gain": scatter_about(part_keys[2], (CH,), 1.0, 4.0, ((0, 2),), jnp.float32),
        "gate_values": scatter_about(part_keys[3], (SEQS, NEW, CH), 1.0, 6.0, ((0, 2), (1, 4), (2, 2))),
    }


def reference(history, filter_taps, skip_gain, gate_values):
    full_len = history.shape[1]
    fft_len = 2 * full_len
    channels = history.shape[2]
    width = min(256, channels)
    blocks = channels // width
    inputs = history.reshape(history.shape[0], full_len, blocks, width).transpose(2, 0, 1, 3)
    filters = filter_taps[::-1].reshape(full_len, blocks, width).transpose(1, 0, 2)

    def per_block(pair):
        values, taps = pair
        spectrum_in = jnp.fft.rfft(values.astype(jnp.float32), n=fft_len, axis=1)
        spectrum_taps = jnp.fft.rfft(taps.astype(jnp.float32), n=fft_len, axis=0)
        result = jnp.fft.irfft(spectrum_in * spectrum_taps[None], n=fft_len, axis=1)
        return result[:, full_len - NEW:full_len].astype(jnp.float32)

    conv = lax.map(per_block, (inputs, filters))
    conv = conv.transpose(1, 2, 0, 3).reshape(history.shape[0], NEW, channels)
    newest = history[:, full_len - NEW:, :].astype(jnp.float32)
    mixed = conv + skip_gain[None, None, :] * newest
    return (gate_values.astype(jnp.float32) * mixed).astype(jnp.bfloat16)
```

```python
import functools
import math

import jax
import jax.numpy as jnp
import numpy as np
from jax import lax
from jax.experimental import pallas as pl
from jax.experimental.pallas import tpu as pltpu
from jax.sharding import PartitionSpec as P

MESH = pl.DeviceIdType.MESH
F32 = jnp.float32
BF16 = jnp.bfloat16
LAG = 2
GAP = 4
DEPTH = 2


def tables(new, piece):
    length = piece + new
    freqs = 2 * np.arange(length // 2)[:, None] + 1

    def both(times):
        angle = math.pi / length * (freqs * times[None, :] % (2 * length))
        pairs = np.stack([np.cos(angle), np.sin(angle)]).reshape(2, -1, 16, times.size)
        return pairs.transpose(1, 0, 2, 3).reshape(length, times.size)

    taps_table = both(np.arange(length))
    data_table = both(np.arange(piece))
    back_table = both(new - 1 - np.arange(new)).T * (2.0 / length)
    return [jnp.asarray(table, BF16) for table in (taps_table, data_table, back_table)]


def kernel(
    n, new, piece, width,
    ft_hbm, fh_hbm, fi_hbm, hist_hbm, taps_hbm, gain_hbm, gate_hbm, out_hbm,
    ft, fh, fi, hist, taps, gain, gate, out, tspec, dspec, spec, part,
    send, recv, in_sem, small_sem, out_sem, rim_sem, pass_sem, open_sem, send_sem, recv_sem,
):
    me = lax.axis_index("hist")
    core, cores = lax.axis_index("seq"), lax.axis_size("seq")
    right, left = me + 1, me - 1
    first, last = me == 0, me == n - 1
    chunks, seqs, block, _ = hist.shape
    own = new // n
    bins = (piece + new) // 2
    pieces = block // piece
    direct = chunks // cores
    ends = n - 1 - me

    def lanes(i):
        c = lax.rem(i + core * direct, chunks)
        return pl.ds(pl.multiple_of(c * width, width), width)

    small = [
        pltpu.make_async_copy(source, target, small_sem.at[i])
        for i, (source, target) in enumerate(
            [(ft_hbm, ft), (fh_hbm, fh), (fi_hbm, fi), (gain_hbm, gain), (gate_hbm, gate)]
        )
    ]

    def load_taps(i):
        return pltpu.make_async_copy(
            taps_hbm.at[:, lanes(i)], taps.at[i, pl.ds(0, block)], in_sem.at[0, i]
        )

    def load_hist(i):
        return pltpu.make_async_copy(hist_hbm.at[:, :, lanes(i)], hist.at[i], in_sem.at[1, i])

    def store(i):
        return pltpu.make_async_copy(out.at[i], out_hbm.at[:, :, lanes(i)], out_sem.at[i])

    def rim_copy(i):
        return pltpu.make_async_remote_copy(
            src_ref=taps_hbm.at[pl.ds(0, new), lanes(i)],
            dst_ref=taps.at[i, pl.ds(block, new)],
            send_sem=rim_sem.at[0, i],
            recv_sem=rim_sem.at[1, i],
            device_id={"hist": left},
            device_id_type=MESH,
        )

    def rim_pass(i, far):
        j = i + far * direct
        return pltpu.make_async_remote_copy(
            src_ref=taps.at[i, pl.ds(block, new)],
            dst_ref=taps.at[j, pl.ds(block, new)],
            send_sem=pass_sem.at[far - 1, i],
            recv_sem=rim_sem.at[1, j],
            device_id={"seq": lax.rem(core + cores - far, cores)},
            device_id_type=MESH,
        )

    def hop(way, owner, i):
        return pltpu.make_async_remote_copy(
            src_ref=send.at[way, owner, i],
            dst_ref=recv.at[way, owner, i],
            send_sem=send_sem.at[way, owner, i],
            recv_sem=recv_sem.at[way, owner, i],
            device_id={"hist": right if way == 0 else left},
            device_id_type=MESH,
        )

    for copy in small[:3]:
        copy.start()

    def start_loads(i, carry):
        load_taps(i).start()
        load_hist(i).start()
        return carry

    lax.fori_loop(0, min(DEPTH, chunks), start_loads, 0)
    for copy in small[3:]:
        copy.start()

    barrier = pltpu.get_barrier_semaphore()

    @pl.when(jnp.logical_not(last))
    def _():
        pl.semaphore_signal(barrier, inc=1, device_id={"hist": right}, device_id_type=MESH)

    for far in range(1, cores):
        pl.semaphore_signal(
            barrier, inc=1, device_id={"seq": lax.rem(core + far, cores)}, device_id_type=MESH
        )
    pl.semaphore_wait(barrier, cores - first.astype(jnp.int32))

    def start_rims(i, carry):
        rim_copy(i).start()
        return carry

    @pl.when(jnp.logical_not(first))
    def _():
        pl.semaphore_signal(open_sem, inc=1, device_id={"hist": left}, device_id_type=MESH)
        lax.fori_loop(0, direct, start_rims, 0)

    for copy in small:
        copy.wait()
    latest = last.astype(F32)

    def arrive(i):
        @pl.when(i + DEPTH < chunks)
        def _():
            start_loads(i + DEPTH, 0)

        load_taps(i).wait()
        load_hist(i).wait()

    def arrive_rim(i):
        @pl.when(jnp.logical_not(last))
        def _():
            rim_copy(i).wait_recv()

            @pl.when(i < direct)
            def _():
                for far in range(1, cores):
                    rim_pass(i, far).start()

        @pl.when(last)
        def _():
            taps[i, pl.ds(block, new)] = jnp.zeros((new, width), BF16)

    def transform(i, b, slot):
        for q in range(pieces):
            dspec[slot, b, q] = jnp.dot(
                fh[...], hist[i, b, pl.ds(q * piece, piece)], preferred_element_type=F32
            )

    def transform_taps(i, q, slot):
        tspec[slot, q] = jnp.dot(
            ft[...], taps[i, pl.ds(q * piece, piece + new)], preferred_element_type=F32
        )

    def compute(i, slot):
        gains = gain[:, lanes(i)] * latest
        ahead = jnp.minimum(i + 1, chunks - 1)
        for b in range(max(seqs, pieces)):
            if b < seqs:
                transform(ahead, b, 1 - slot)
            if b < pieces:
                transform_taps(ahead, b, 1 - slot)
            if b >= seqs:
                continue
            for r in range(0, bins, 16):
                low, high = pl.ds(2 * r, 16), pl.ds(2 * r + 16, 16)
                real = imag = None
                for q in range(pieces):
                    hc, hs = dspec[slot, b, q, low], dspec[slot, b, q, high]
                    tc, ts = tspec[slot, q, low], tspec[slot, q, high]
                    one, two = tc * hc + ts * hs, ts * hc - tc * hs
                    real = one if q == 0 else real + one
                    imag = two if q == 0 else imag + two
                spec[b, low] = real.astype(BF16)
                spec[b, high] = imag.astype(BF16)
            value = jnp.dot(fi[...], spec[b], preferred_element_type=F32)
            value = value + gains * hist[i, b, pl.ds(block - new, new)].astype(F32)
            for d in range(n):
                part[i, d, b] = value[d * own : (d + 1) * own]

    def pass_on(way, owner, i):
        edge = first if way == 0 else last

        @pl.when(edge)
        def _():
            for b in range(seqs):
                send[way, owner, i, b] = part[i, owner, b].astype(BF16)

        @pl.when(jnp.logical_not(edge))
        def _():
            hop(way, owner, i).wait_recv()
            for b in range(seqs):
                value = part[i, owner, b] + recv[way, owner, i, b].astype(F32)
                send[way, owner, i, b] = value.astype(BF16)

        hop(way, owner, i).start()

    def finish(i):
        @pl.when(jnp.logical_not(first))
        def _():
            hop(0, me, i).wait_recv()
            for b in range(seqs):
                part[i, me, b] += recv[0, me, i, b].astype(F32)

        @pl.when(jnp.logical_not(last))
        def _():
            hop(1, me, i).wait_recv()
            for b in range(seqs):
                part[i, me, b] += recv[1, me, i, b].astype(F32)

        for b in range(seqs):
            out_hbm[b, :, lanes(i)] = (gate[b, :, lanes(i)].astype(F32) * part[i, me, b]).astype(BF16)

    def guarded(i, action):
        @pl.when(jnp.logical_and(i >= 0, i < chunks))
        def _():
            action(i)

    def turn(k):
        return GAP * k + jnp.where(k == n - 2, chunks - GAP, 0)

    final = jnp.where(
        jnp.logical_or(first, last),
        chunks + turn(n - 2),
        jnp.maximum(LAG * ends + turn(me), LAG * me + turn(ends)),
    )

    def step(t, slot):
        @pl.when(t + 1 < chunks)
        def _():
            arrive(t + 1)
            arrive_rim(t + 1)

        @pl.when(t < chunks)
        def _():
            compute(t, slot)

        def to_left(k, carry):
            guarded(t - LAG * ends - turn(k), functools.partial(pass_on, 1, k))
            return carry

        def to_right(k, carry):
            guarded(t - LAG * me - turn(k), functools.partial(pass_on, 0, n - 1 - k))
            return carry

        lax.fori_loop(0, me, to_left, 0)
        lax.fori_loop(0, ends, to_right, 0)
        guarded(t - final, finish)

    def steps(p, carry):
        for slot in range(2):
            step(2 * p + slot, slot)
        return carry

    arrive(0)
    for b in range(seqs):
        transform(0, b, 0)
    arrive_rim(0)
    for q in range(pieces):
        transform_taps(0, q, 0)

    @pl.when(jnp.logical_not(last))
    def _():
        pl.semaphore_wait(open_sem, 1)

    lax.fori_loop(0, (chunks + final + 1) // 2, steps, 0)

    def drain(i, carry):

        @pl.when(jnp.logical_and(i < direct, jnp.logical_not(first)))
        def _():
            rim_copy(i).wait_send()

        @pl.when(jnp.logical_and(i < direct, jnp.logical_not(last)))
        def _():
            for far in range(1, cores):
                rim_pass(i, far).wait_send()

        def drain_left(k, carry):
            hop(1, k, i).wait_send()
            return carry

        def drain_right(k, carry):
            hop(0, n - 1 - k, i).wait_send()
            return carry

        lax.fori_loop(0, me, drain_left, 0)
        lax.fori_loop(0, ends, drain_right, 0)
        return carry

    lax.fori_loop(0, chunks, drain, 0)


def body(history, filter_taps, skip_gain, gate_values):
    n = lax.axis_size("hist")
    seqs, block, channels = history.shape
    own = gate_values.shape[1]
    new = own * n
    piece = min(2 * new, block)
    width = min(256, channels)
    chunks = channels // width
    length = piece + new
    cores = lax.axis_size("seq")
    hbm = pl.BlockSpec(memory_space=pl.ANY)
    return pl.pallas_call(
        functools.partial(kernel, n, new, piece, width),
        out_shape=pltpu.VMEM(gate_values.shape, BF16),
        in_specs=[hbm] * 7,
        out_specs=pl.BlockSpec(memory_space=pltpu.VMEM),
        scratch_shapes=[
            pltpu.VMEM((length, length), BF16),
            pltpu.VMEM((length, piece), BF16),
            pltpu.VMEM((new, length), BF16),
            pltpu.VMEM((chunks, seqs, block, width), BF16),
            pltpu.VMEM((chunks, block + new, width), BF16),
            pltpu.VMEM((1, channels), F32),
            pltpu.VMEM(gate_values.shape, BF16),
            pltpu.VMEM((chunks, seqs, own, width), BF16),
            pltpu.VMEM((2, block // piece, length, width), F32),
            pltpu.VMEM((2, seqs, block // piece, length, width), F32),
            pltpu.VMEM((seqs, length, width), BF16),
            pltpu.VMEM((chunks, n, seqs, own, width), F32),
            pltpu.VMEM((2, n, chunks, seqs, own, width), BF16),
            pltpu.VMEM((2, n, chunks, seqs, own, width), BF16),
            pltpu.SemaphoreType.DMA((2, chunks)),
            pltpu.SemaphoreType.DMA((5,)),
            pltpu.SemaphoreType.DMA((chunks,)),
            pltpu.SemaphoreType.DMA((2, chunks)),
            pltpu.SemaphoreType.DMA((max(cores - 1, 1), chunks // cores)),
            pltpu.SemaphoreType.REGULAR,
            pltpu.SemaphoreType.DMA((2, n, chunks)),
            pltpu.SemaphoreType.DMA((2, n, chunks)),
        ],
        compiler_params=pltpu.CompilerParams(
            collective_id=0, has_side_effects=True, vmem_limit_bytes=60 * 2**20
        ),
    )(*tables(new, piece), history, filter_taps, skip_gain[None, :], gate_values)


def solution(mesh):
    placed = (
        P(("grp", "seq"), "hist", "chan"),
        P(("grp", "hist"), "chan"),
        P(("grp", "chan")),
        P(("grp", "seq"), "hist", "chan"),
    )
    return jax.shard_map(
        body,
        mesh=mesh,
        in_specs=placed,
        out_specs=P(("grp", "seq"), "hist", "chan"),
        check_vma=False,
    )
```

```python
import functools
import math

import jax
import jax.numpy as jnp
import numpy as np
from jax import lax
from jax.experimental import pallas as pl
from jax.experimental.pallas import tpu as pltpu
from jax.sharding import PartitionSpec as P

MESH = pl.DeviceIdType.MESH
F32 = jnp.float32
BF16 = jnp.bfloat16
HOP = 3
LEFT_GAP = 5
RIGHT_GAP = 2
DEPTH = 2


def tables(new, piece):
    length = piece + new
    freqs = 2 * np.arange(length // 2)[:, None] + 1

    def both(times):
        angle = math.pi / length * (freqs * times[None, :] % (2 * length))
        pairs = np.stack([np.cos(angle), np.sin(angle)]).reshape(2, -1, 16, times.size)
        return pairs.transpose(1, 0, 2, 3).reshape(length, times.size)

    taps_table = both(np.arange(length))
    data_table = both(np.arange(piece))
    back_table = both(new - 1 - np.arange(new)).T * (2.0 / length)
    return [jnp.asarray(table, BF16) for table in (taps_table, data_table, back_table)]


def kernel(
    n, new, piece, width,
    ft_hbm, fh_hbm, fi_hbm, hist_hbm, taps_hbm, gain_hbm, gate_hbm, total,
    ft, fh, fi, hist, taps, gain, gate, tspec, dspec, spec, part,
    send, recv, in_sem, small_sem, rim_sem, pass_sem, open_sem, send_sem, recv_sem,
):
    me = lax.axis_index("hist")
    core, cores = lax.axis_index("seq"), lax.axis_size("seq")
    right, left = me + 1, me - 1
    first, last = me == 0, me == n - 1
    chunks, seqs, block, _ = hist.shape
    own = new // n
    bins = (piece + new) // 2
    pieces = block // piece
    direct = chunks // cores
    ends = n - 1 - me

    def lanes(i):
        c = lax.rem(i + core * direct, chunks)
        return pl.ds(pl.multiple_of(c * width, width), width)

    small = [
        pltpu.make_async_copy(source, target, small_sem.at[i])
        for i, (source, target) in enumerate(
            [(ft_hbm, ft), (fh_hbm, fh), (fi_hbm, fi), (gain_hbm, gain), (gate_hbm, gate)]
        )
    ]

    def load_taps(i):
        return pltpu.make_async_copy(
            taps_hbm.at[:, lanes(i)],
            taps.at[i, pl.ds(0, block)],
            in_sem.at[0, lax.rem(i, DEPTH + 1)],
        )

    def load_hist(i):
        return pltpu.make_async_copy(
            hist_hbm.at[:, :, lanes(i)], hist.at[i], in_sem.at[1, lax.rem(i, DEPTH + 1)]
        )

    def rim(source, target, i):
        return pltpu.make_async_remote_copy(
            src_ref=source,
            dst_ref=target,
            send_sem=pass_sem.at[0],
            recv_sem=rim_sem.at[i],
            device_id={"hist": left},
            device_id_type=MESH,
        )

    def rim_copy(i):
        return rim(taps_hbm.at[pl.ds(0, new), lanes(i)], taps.at[i, pl.ds(block, new)], i)

    def rim_pass(i, far):
        j = i + far * direct
        return pltpu.make_async_remote_copy(
            src_ref=taps.at[i, pl.ds(block, new)],
            dst_ref=taps.at[j, pl.ds(block, new)],
            send_sem=pass_sem.at[far],
            recv_sem=rim_sem.at[j],
            device_id={"seq": lax.rem(core + cores - far, cores)},
            device_id_type=MESH,
        )

    def all_passed(far):
        rims = taps.at[pl.ds(0, direct), pl.ds(block, new)]
        return pltpu.make_async_remote_copy(
            src_ref=rims,
            dst_ref=rims,
            send_sem=pass_sem.at[far],
            recv_sem=rim_sem.at[0],
            device_id={"hist": left},
            device_id_type=MESH,
        )

    def hop(way, owner, i):
        return pltpu.make_async_remote_copy(
            src_ref=send.at[owner, i],
            dst_ref=recv.at[owner + 1 - way, i],
            send_sem=send_sem.at[owner],
            recv_sem=recv_sem.at[owner + 1 - way, i],
            device_id={"hist": right if way == 0 else left},
            device_id_type=MESH,
        )

    def all_sent(owner):
        return pltpu.make_async_remote_copy(
            src_ref=send.at[owner],
            dst_ref=recv.at[owner],
            send_sem=send_sem.at[owner],
            recv_sem=recv_sem.at[owner, 0],
            device_id={"hist": right},
            device_id_type=MESH,
        )

    for copy in small[:3]:
        copy.start()

    def start_loads(i, carry):
        load_taps(i).start()
        load_hist(i).start()
        return carry

    lax.fori_loop(0, min(DEPTH, chunks), start_loads, 0)
    for copy in small[3:]:
        copy.start()

    barrier = pltpu.get_barrier_semaphore()

    @pl.when(jnp.logical_not(last))
    def _():
        pl.semaphore_signal(barrier, inc=1, device_id={"hist": right}, device_id_type=MESH)

    for other in range(1, cores):
        @pl.when(core < other)
        def _():
            pl.semaphore_signal(barrier, inc=1, device_id={"seq": other}, device_id_type=MESH)

    greeted = core + 1 - first.astype(jnp.int32)

    @pl.when(greeted > 0)
    def _():
        pl.semaphore_wait(barrier, greeted)

    def start_rims(i, carry):
        rim_copy(i).start()
        return carry

    @pl.when(jnp.logical_not(first))
    def _():
        pl.semaphore_signal(open_sem.at[0], inc=1, device_id={"hist": left}, device_id_type=MESH)
        lax.fori_loop(0, direct, start_rims, 0)

    for other in range(cores - 1):
        @pl.when(core > other)
        def _():
            pl.semaphore_signal(
                open_sem.at[1], inc=1, device_id={"seq": other}, device_id_type=MESH
            )

    for copy in small:
        copy.wait()
    latest = last.astype(F32)

    def arrive(i):
        @pl.when(i + DEPTH < chunks)
        def _():
            start_loads(i + DEPTH, 0)

        load_taps(i).wait()
        load_hist(i).wait()

    def arrive_rim(i):
        @pl.when(jnp.logical_not(last))
        def _():
            rim_copy(i).wait_recv()

            @pl.when(i < direct)
            def _():
                for far in range(1, cores):
                    rim_pass(i, far).start()

        @pl.when(last)
        def _():
            taps[i, pl.ds(block, new)] = jnp.zeros((new, width), BF16)

    def transform(i, b, slot):
        for q in range(pieces):
            dspec[slot, b, q] = jnp.dot(
                fh[...], hist[i, b, pl.ds(q * piece, piece)], preferred_element_type=F32
            )

    def transform_taps(i, q, slot):
        tspec[slot, q] = jnp.dot(
            ft[...], taps[i, pl.ds(q * piece, piece + new)], preferred_element_type=F32
        )

    def compute(i, slot):
        gains = gain[:, lanes(i)] * latest
        ahead = jnp.minimum(i + 1, chunks - 1)
        for b in range(max(seqs, pieces)):
            if b < seqs:
                transform(ahead, b, 1 - slot)
            if b < pieces:
                transform_taps(ahead, b, 1 - slot)
            if b >= seqs:
                continue
            for r in range(0, bins, 16):
                low, high = pl.ds(2 * r, 16), pl.ds(2 * r + 16, 16)
                real = imag = None
                for q in range(pieces):
                    hc, hs = dspec[slot, b, q, low], dspec[slot, b, q, high]
                    tc, ts = tspec[slot, q, low], tspec[slot, q, high]
                    one, two = tc * hc + ts * hs, ts * hc - tc * hs
                    real = one if q == 0 else real + one
                    imag = two if q == 0 else imag + two
                spec[b, low] = real.astype(BF16)
                spec[b, high] = imag.astype(BF16)
            value = jnp.dot(fi[...], spec[b], preferred_element_type=F32)
            value = value + gains * hist[i, b, pl.ds(block - new, new)].astype(F32)
            for d in range(n):
                part[i, d, b] = value[d * own : (d + 1) * own]

    def pass_on(way, owner, i):
        edge = first if way == 0 else last

        @pl.when(edge)
        def _():
            for b in range(seqs):
                send[owner, i, b] = part[i, owner, b].astype(BF16)

        @pl.when(jnp.logical_not(edge))
        def _():
            hop(way, owner, i).wait_recv()
            for b in range(seqs):
                value = part[i, owner, b] + recv[owner + 1 - way, i, b].astype(F32)
                send[owner, i, b] = value.astype(BF16)

        hop(way, owner, i).start()

    def finish(i):
        @pl.when(jnp.logical_not(first))
        def _():
            hop(0, me, i).wait_recv()
            for b in range(seqs):
                part[i, me, b] += recv[me + 1, i, b].astype(F32)

        @pl.when(jnp.logical_not(last))
        def _():
            hop(1, me, i).wait_recv()
            for b in range(seqs):
                part[i, me, b] += recv[me, i, b].astype(F32)

        for b in range(seqs):
            total[b, :, lanes(i)] = (gate[b, :, lanes(i)].astype(F32) * part[i, me, b]).astype(BF16)

    def guarded(i, action):
        @pl.when(jnp.logical_and(i >= 0, i < chunks))
        def _():
            action(i)

    def turn(way, k):
        gap = RIGHT_GAP if way == 0 else LEFT_GAP
        return gap * k + jnp.where(k == n - 2, chunks - gap, 0)

    left_lag = jnp.where(last, 0, HOP * ends - 1)
    right_lag = jnp.where(first, 0, HOP * me + 1)
    final = jnp.where(
        jnp.logical_or(first, last),
        jnp.maximum(chunks + jnp.maximum(turn(0, n - 2), turn(1, n - 2)), HOP * n),
        jnp.maximum(left_lag + turn(1, me), right_lag + turn(0, ends)),
    )

    def step(t, slot):
        @pl.when(t + 1 < chunks)
        def _():
            arrive(t + 1)
            arrive_rim(t + 1)

        @pl.when(t < chunks)
        def _():
            compute(t, slot)

        def to_left(k, carry):
            guarded(t - left_lag - turn(1, k), functools.partial(pass_on, 1, k))
            return carry

        def to_right(k, carry):
            guarded(t - right_lag - turn(0, k), functools.partial(pass_on, 0, n - 1 - k))
            return carry

        lax.fori_loop(0, me, to_left, 0)
        lax.fori_loop(0, ends, to_right, 0)
        guarded(t - final, finish)

    def steps(p, carry):
        for slot in range(2):
            step(2 * p + slot, slot)
        return carry

    arrive(0)
    for b in range(seqs):
        transform(0, b, 0)
    for q in range(pieces - 1):
        transform_taps(0, q, 0)

    @pl.when(core < cores - 1)
    def _():
        pl.semaphore_wait(open_sem.at[1], cores - 1 - core)

    arrive_rim(0)
    transform_taps(0, pieces - 1, 0)

    @pl.when(jnp.logical_not(last))
    def _():
        pl.semaphore_wait(open_sem.at[0], 1)

    lax.fori_loop(0, (chunks + final + 1) // 2, steps, 0)

    @pl.when(jnp.logical_not(first))
    def _():
        all_passed(0).wait_send()

    @pl.when(jnp.logical_not(last))
    def _():
        for far in range(1, cores):
            all_passed(far).wait_send()

    def drain(owner, carry):
        @pl.when(owner != me)
        def _():
            all_sent(owner).wait_send()

        return carry

    lax.fori_loop(0, n, drain, 0)


def body(history, filter_taps, skip_gain, gate_values):
    n = lax.axis_size("hist")
    seqs, block, channels = history.shape
    own = gate_values.shape[1]
    new = own * n
    piece = min(2 * new, block)
    width = min(256, channels)
    chunks = channels // width
    length = piece + new
    cores = lax.axis_size("seq")
    hbm = pl.BlockSpec(memory_space=pl.ANY)
    return pl.pallas_call(
        functools.partial(kernel, n, new, piece, width),
        out_shape=pltpu.VMEM(gate_values.shape, BF16),
        in_specs=[hbm] * 7,
        out_specs=pl.BlockSpec(memory_space=pltpu.VMEM),
        scratch_shapes=[
            pltpu.VMEM((length, length), BF16),
            pltpu.VMEM((length, piece), BF16),
            pltpu.VMEM((new, length), BF16),
            pltpu.VMEM((chunks, seqs, block, width), BF16),
            pltpu.VMEM((chunks, block + new, width), BF16),
            pltpu.VMEM((1, channels), F32),
            pltpu.VMEM(gate_values.shape, BF16),
            pltpu.VMEM((2, block // piece, length, width), F32),
            pltpu.VMEM((2, seqs, block // piece, length, width), F32),
            pltpu.VMEM((seqs, length, width), BF16),
            pltpu.VMEM((chunks, n, seqs, own, width), F32),
            pltpu.VMEM((n, chunks, seqs, own, width), BF16),
            pltpu.VMEM((n + 1, chunks, seqs, own, width), BF16),
            pltpu.SemaphoreType.DMA((2, DEPTH + 1)),
            pltpu.SemaphoreType.DMA((5,)),
            pltpu.SemaphoreType.DMA((chunks,)),
            pltpu.SemaphoreType.DMA((cores,)),
            pltpu.SemaphoreType.REGULAR((2,)),
            pltpu.SemaphoreType.DMA((n,)),
            pltpu.SemaphoreType.DMA((n + 1, chunks)),
        ],
        compiler_params=pltpu.CompilerParams(
            collective_id=0, has_side_effects=True, vmem_limit_bytes=60 * 2**20
        ),
    )(*tables(new, piece), history, filter_taps, skip_gain[None, :], gate_values)


def solution(mesh):
    placed = (
        P(("grp", "seq"), "hist", "chan"),
        P(("grp", "hist"), "chan"),
        P(("grp", "chan")),
        P(("grp", "seq"), "hist", "chan"),
    )
    return jax.shard_map(
        body,
        mesh=mesh,
        in_specs=placed,
        out_specs=P(("grp", "seq"), "hist", "chan"),
        check_vma=False,
    )
```

```python
import functools
import math

import jax
import jax.numpy as jnp
import numpy as np
from jax import lax
from jax.experimental import pallas as pl
from jax.experimental.pallas import tpu as pltpu
from jax.sharding import PartitionSpec as P

MESH = pl.DeviceIdType.MESH
F32 = jnp.float32
BF16 = jnp.bfloat16
LEFT_HOP = 3
LEFT_GAP = 5
RIGHT_GAP = 0
RIGHT_HOP = 4
DEPTH = 2


def tables(new, piece):
    length = piece + new
    freqs = 2 * np.arange(length // 2)[:, None] + 1

    def both(times):
        angle = math.pi / length * (freqs * times[None, :] % (2 * length))
        pairs = np.stack([np.cos(angle), np.sin(angle)]).reshape(2, -1, 16, times.size)
        return pairs.transpose(1, 0, 2, 3).reshape(length, times.size)

    taps_table = both(np.arange(length))
    data_table = both(np.arange(piece))
    back_table = both(new - 1 - np.arange(new)).T * (2.0 / length)
    return [jnp.asarray(table, BF16) for table in (taps_table, data_table, back_table)]


def kernel(
    n, new, piece, width,
    ft_hbm, fh_hbm, fi_hbm, hist_hbm, taps_hbm, gain_hbm, gate_hbm, total,
    ft, fh, fi, hist, taps, gain, gate, tspec, dspec, spec, part,
    send, recv, in_sem, small_sem, rim_sem, pass_sem, open_sem, send_sem, recv_sem,
):
    me = lax.axis_index("hist")
    core, cores = lax.axis_index("seq"), lax.axis_size("seq")
    right, left = me + 1, me - 1
    first, last = me == 0, me == n - 1
    chunks, seqs, block, _ = hist.shape
    own = new // n
    bins = (piece + new) // 2
    pieces = block // piece
    direct = chunks // cores
    ends = n - 1 - me

    def lanes(i):
        c = lax.rem(i + core * direct, chunks)
        return pl.ds(pl.multiple_of(c * width, width), width)

    small = [
        pltpu.make_async_copy(source, target, small_sem.at[i])
        for i, (source, target) in enumerate(
            [(ft_hbm, ft), (fh_hbm, fh), (fi_hbm, fi), (gain_hbm, gain), (gate_hbm, gate)]
        )
    ]

    def load_taps(i):
        return pltpu.make_async_copy(
            taps_hbm.at[:, lanes(i)],
            taps.at[i, pl.ds(0, block)],
            in_sem.at[0, lax.rem(i, DEPTH + 1)],
        )

    def load_hist(i):
        return pltpu.make_async_copy(
            hist_hbm.at[:, :, lanes(i)], hist.at[i], in_sem.at[1, lax.rem(i, DEPTH + 1)]
        )

    def rim(source, target, i):
        return pltpu.make_async_remote_copy(
            src_ref=source,
            dst_ref=target,
            send_sem=pass_sem.at[0],
            recv_sem=rim_sem.at[i],
            device_id={"hist": left},
            device_id_type=MESH,
        )

    def rim_copy(i):
        return rim(taps_hbm.at[pl.ds(0, new), lanes(i)], taps.at[i, pl.ds(block, new)], i)

    def rim_pass(i, far):
        j = i + far * direct
        return pltpu.make_async_remote_copy(
            src_ref=taps.at[i, pl.ds(block, new)],
            dst_ref=taps.at[j, pl.ds(block, new)],
            send_sem=pass_sem.at[far],
            recv_sem=rim_sem.at[j],
            device_id={"seq": lax.rem(core + cores - far, cores)},
            device_id_type=MESH,
        )

    def all_passed(far):
        rims = taps.at[pl.ds(0, direct), pl.ds(block, new)]
        return pltpu.make_async_remote_copy(
            src_ref=rims,
            dst_ref=rims,
            send_sem=pass_sem.at[far],
            recv_sem=rim_sem.at[0],
            device_id={"hist": left},
            device_id_type=MESH,
        )

    def hop(way, owner, i):
        return pltpu.make_async_remote_copy(
            src_ref=send.at[owner, i],
            dst_ref=recv.at[owner + 1 - way, i],
            send_sem=send_sem.at[owner],
            recv_sem=recv_sem.at[owner + 1 - way, i],
            device_id={"hist": right if way == 0 else left},
            device_id_type=MESH,
        )

    def all_sent(owner):
        return pltpu.make_async_remote_copy(
            src_ref=send.at[owner],
            dst_ref=recv.at[owner],
            send_sem=send_sem.at[owner],
            recv_sem=recv_sem.at[owner, 0],
            device_id={"hist": right},
            device_id_type=MESH,
        )

    for copy in small[:3]:
        copy.start()

    def start_loads(i, carry):
        load_taps(i).start()
        load_hist(i).start()
        return carry

    lax.fori_loop(0, min(DEPTH, chunks), start_loads, 0)
    for copy in small[3:]:
        copy.start()

    barrier = pltpu.get_barrier_semaphore()

    @pl.when(jnp.logical_not(last))
    def _():
        pl.semaphore_signal(barrier, inc=1, device_id={"hist": right}, device_id_type=MESH)

    for other in range(1, cores):
        @pl.when(core < other)
        def _():
            pl.semaphore_signal(barrier, inc=1, device_id={"seq": other}, device_id_type=MESH)

    greeted = core + 1 - first.astype(jnp.int32)

    @pl.when(greeted > 0)
    def _():
        pl.semaphore_wait(barrier, greeted)

    def start_rims(i, carry):
        rim_copy(i).start()
        return carry

    @pl.when(jnp.logical_not(first))
    def _():
        pl.semaphore_signal(open_sem.at[0], inc=1, device_id={"hist": left}, device_id_type=MESH)
        lax.fori_loop(0, direct, start_rims, 0)

    for other in range(cores - 1):
        @pl.when(core > other)
        def _():
            pl.semaphore_signal(
                open_sem.at[1], inc=1, device_id={"seq": other}, device_id_type=MESH
            )

    for copy in small:
        copy.wait()
    latest = last.astype(F32)

    def arrive(i):
        @pl.when(i + DEPTH < chunks)
        def _():
            start_loads(i + DEPTH, 0)

        load_taps(i).wait()
        load_hist(i).wait()

    def arrive_rim(i):
        @pl.when(jnp.logical_not(last))
        def _():
            rim_copy(i).wait_recv()

            @pl.when(i < direct)
            def _():
                for far in range(1, cores):
                    rim_pass(i, far).start()

        @pl.when(last)
        def _():
            taps[i, pl.ds(block, new)] = jnp.zeros((new, width), BF16)

    def transform(i, b, slot):
        for q in range(pieces):
            dspec[slot, b, q] = jnp.dot(
                fh[...], hist[i, b, pl.ds(q * piece, piece)], preferred_element_type=F32
            )

    def transform_taps(i, q, slot):
        tspec[slot, q] = jnp.dot(
            ft[...], taps[i, pl.ds(q * piece, piece + new)], preferred_element_type=F32
        )

    def compute(i, slot):
        gains = gain[:, lanes(i)] * latest
        ahead = jnp.minimum(i + 1, chunks - 1)
        for b in range(max(seqs, pieces)):
            if b < seqs:
                transform(ahead, b, 1 - slot)
            if b < pieces:
                transform_taps(ahead, b, 1 - slot)
            if b >= seqs:
                continue
            for r in range(0, bins, 16):
                low, high = pl.ds(2 * r, 16), pl.ds(2 * r + 16, 16)
                real = imag = None
                for q in range(pieces):
                    hc, hs = dspec[slot, b, q, low], dspec[slot, b, q, high]
                    tc, ts = tspec[slot, q, low], tspec[slot, q, high]
                    one, two = tc * hc + ts * hs, ts * hc - tc * hs
                    real = one if q == 0 else real + one
                    imag = two if q == 0 else imag + two
                spec[b, low] = real.astype(BF16)
                spec[b, high] = imag.astype(BF16)
            value = jnp.dot(fi[...], spec[b], preferred_element_type=F32)
            value = value + gains * hist[i, b, pl.ds(block - new, new)].astype(F32)
            for d in range(n):
                part[i, d, b] = value[d * own : (d + 1) * own]

    def pass_on(way, owner, i):
        edge = first if way == 0 else last

        @pl.when(edge)
        def _():
            for b in range(seqs):
                send[owner, i, b] = part[i, owner, b].astype(BF16)

        @pl.when(jnp.logical_not(edge))
        def _():
            hop(way, owner, i).wait_recv()
            for b in range(seqs):
                value = part[i, owner, b] + recv[owner + 1 - way, i, b].astype(F32)
                send[owner, i, b] = value.astype(BF16)

        hop(way, owner, i).start()

    def finish(i):
        @pl.when(jnp.logical_not(first))
        def _():
            hop(0, me, i).wait_recv()
            for b in range(seqs):
                part[i, me, b] += recv[me + 1, i, b].astype(F32)

        @pl.when(jnp.logical_not(last))
        def _():
            hop(1, me, i).wait_recv()
            for b in range(seqs):
                part[i, me, b] += recv[me, i, b].astype(F32)

        for b in range(seqs):
            total[b, :, lanes(i)] = (gate[b, :, lanes(i)].astype(F32) * part[i, me, b]).astype(BF16)

    def guarded(i, action):
        @pl.when(jnp.logical_and(i >= 0, i < chunks))
        def _():
            action(i)

    def turn(way, k):
        gap = RIGHT_GAP if way == 0 else LEFT_GAP
        return gap * k + jnp.where(k == n - 2, chunks - gap, 0)

    left_lag = jnp.where(last, 0, LEFT_HOP * ends - 1)
    right_lag = jnp.where(first, 0, RIGHT_HOP * me)
    final = jnp.where(
        jnp.logical_or(first, last),
        jnp.maximum(chunks + jnp.maximum(turn(0, n - 2), turn(1, n - 2)), max(LEFT_HOP, RIGHT_HOP) * n),
        jnp.maximum(left_lag + turn(1, me), right_lag + turn(0, ends)),
    )

    def step(t, slot):
        @pl.when(t + 1 < chunks)
        def _():
            arrive(t + 1)
            arrive_rim(t + 1)

        @pl.when(t < chunks)
        def _():
            compute(t, slot)

        def to_left(k, carry):
            guarded(t - left_lag - turn(1, k), functools.partial(pass_on, 1, k))
            return carry

        def to_right(k, carry):
            guarded(t - right_lag - turn(0, k), functools.partial(pass_on, 0, n - 1 - k))
            return carry

        lax.fori_loop(0, me, to_left, 0)
        lax.fori_loop(0, ends, to_right, 0)
        guarded(t - final, finish)

    def steps(p, carry):
        for slot in range(2):
            step(2 * p + slot, slot)
        return carry

    arrive(0)
    for b in range(seqs):
        transform(0, b, 0)
    for q in range(pieces - 1):
        transform_taps(0, q, 0)

    @pl.when(core < cores - 1)
    def _():
        pl.semaphore_wait(open_sem.at[1], cores - 1 - core)

    arrive_rim(0)
    transform_taps(0, pieces - 1, 0)

    @pl.when(jnp.logical_not(last))
    def _():
        pl.semaphore_wait(open_sem.at[0], 1)

    lax.fori_loop(0, (chunks + final + 1) // 2, steps, 0)

    @pl.when(jnp.logical_not(first))
    def _():
        all_passed(0).wait_send()

    @pl.when(jnp.logical_not(last))
    def _():
        for far in range(1, cores):
            all_passed(far).wait_send()

    def drain(owner, carry):
        @pl.when(owner != me)
        def _():
            all_sent(owner).wait_send()

        return carry

    lax.fori_loop(0, n, drain, 0)


def body(history, filter_taps, skip_gain, gate_values):
    n = lax.axis_size("hist")
    seqs, block, channels = history.shape
    own = gate_values.shape[1]
    new = own * n
    piece = min(2 * new, block)
    width = min(256, channels)
    chunks = channels // width
    length = piece + new
    cores = lax.axis_size("seq")
    hbm = pl.BlockSpec(memory_space=pl.ANY)
    return pl.pallas_call(
        functools.partial(kernel, n, new, piece, width),
        out_shape=pltpu.VMEM(gate_values.shape, BF16),
        in_specs=[hbm] * 7,
        out_specs=pl.BlockSpec(memory_space=pltpu.VMEM),
        scratch_shapes=[
            pltpu.VMEM((length, length), BF16),
            pltpu.VMEM((length, piece), BF16),
            pltpu.VMEM((new, length), BF16),
            pltpu.VMEM((chunks, seqs, block, width), BF16),
            pltpu.VMEM((chunks, block + new, width), BF16),
            pltpu.VMEM((1, channels), F32),
            pltpu.VMEM(gate_values.shape, BF16),
            pltpu.VMEM((2, block // piece, length, width), F32),
            pltpu.VMEM((2, seqs, block // piece, length, width), F32),
            pltpu.VMEM((seqs, length, width), BF16),
            pltpu.VMEM((chunks, n, seqs, own, width), F32),
            pltpu.VMEM((n, chunks, seqs, own, width), BF16),
            pltpu.VMEM((n + 1, chunks, seqs, own, width), BF16),
            pltpu.SemaphoreType.DMA((2, DEPTH + 1)),
            pltpu.SemaphoreType.DMA((5,)),
            pltpu.SemaphoreType.DMA((chunks,)),
            pltpu.SemaphoreType.DMA((cores,)),
            pltpu.SemaphoreType.REGULAR((2,)),
            pltpu.SemaphoreType.DMA((n,)),
            pltpu.SemaphoreType.DMA((n + 1, chunks)),
        ],
        compiler_params=pltpu.CompilerParams(
            collective_id=0, has_side_effects=True, vmem_limit_bytes=60 * 2**20
        ),
    )(*tables(new, piece), history, filter_taps, skip_gain[None, :], gate_values)


def solution(mesh):
    placed = (
        P(("grp", "seq"), "hist", "chan"),
        P(("grp", "hist"), "chan"),
        P(("grp", "chan")),
        P(("grp", "seq"), "hist", "chan"),
    )
    return jax.shard_map(
        body,
        mesh=mesh,
        in_specs=placed,
        out_specs=P(("grp", "seq"), "hist", "chan"),
        check_vma=False,
    )
```

```python
import functools
import math

import jax
import jax.numpy as jnp
import numpy as np
from jax import lax
from jax.experimental import pallas as pl
from jax.experimental.pallas import tpu as pltpu
from jax.sharding import PartitionSpec as P

MESH = pl.DeviceIdType.MESH
F32 = jnp.float32
BF16 = jnp.bfloat16
LEFT_HOP = 3
LEFT_GAP = 5
OTHER_LEFT_GAP = 3
RIGHT_GAP = 0
RIGHT_HOP = 4
DEPTH = 2


def tables(new, piece):
    length = piece + new
    freqs = 2 * np.arange(length // 2)[:, None] + 1

    def both(times):
        angle = math.pi / length * (freqs * times[None, :] % (2 * length))
        pairs = np.stack([np.cos(angle), np.sin(angle)]).reshape(2, -1, 16, times.size)
        return pairs.transpose(1, 0, 2, 3).reshape(length, times.size)

    taps_table = both(np.arange(length))
    data_table = both(np.arange(piece))
    back_table = both(new - 1 - np.arange(new)).T * (2.0 / length)
    return [jnp.asarray(table, BF16) for table in (taps_table, data_table, back_table)]


def kernel(
    n, new, piece, width,
    ft_hbm, fh_hbm, fi_hbm, hist_hbm, taps_hbm, gain_hbm, gate_hbm, total,
    ft, fh, fi, hist, taps, gain, gate, tspec, dspec, spec, part,
    send, recv, in_sem, small_sem, rim_sem, pass_sem, open_sem, send_sem, recv_sem,
):
    me = lax.axis_index("hist")
    core, cores = lax.axis_index("seq"), lax.axis_size("seq")
    right, left = me + 1, me - 1
    first, last = me == 0, me == n - 1
    chunks, seqs, block, _ = hist.shape
    own = new // n
    bins = (piece + new) // 2
    pieces = block // piece
    direct = chunks // cores
    ends = n - 1 - me

    def lanes(i):
        c = lax.rem(i + core * direct, chunks)
        return pl.ds(pl.multiple_of(c * width, width), width)

    small = [
        pltpu.make_async_copy(source, target, small_sem.at[i])
        for i, (source, target) in enumerate(
            [(ft_hbm, ft), (fh_hbm, fh), (fi_hbm, fi), (gain_hbm, gain), (gate_hbm, gate)]
        )
    ]

    def load_taps(i):
        return pltpu.make_async_copy(
            taps_hbm.at[:, lanes(i)],
            taps.at[i, pl.ds(0, block)],
            in_sem.at[0, lax.rem(i, DEPTH + 1)],
        )

    def load_hist(i):
        return pltpu.make_async_copy(
            hist_hbm.at[:, :, lanes(i)], hist.at[i], in_sem.at[1, lax.rem(i, DEPTH + 1)]
        )

    def rim(source, target, i):
        return pltpu.make_async_remote_copy(
            src_ref=source,
            dst_ref=target,
            send_sem=pass_sem.at[0],
            recv_sem=rim_sem.at[i],
            device_id={"hist": left},
            device_id_type=MESH,
        )

    def rim_copy(i):
        return rim(taps_hbm.at[pl.ds(0, new), lanes(i)], taps.at[i, pl.ds(block, new)], i)

    def rim_pass(i, far):
        j = i + far * direct
        return pltpu.make_async_remote_copy(
            src_ref=taps.at[i, pl.ds(block, new)],
            dst_ref=taps.at[j, pl.ds(block, new)],
            send_sem=pass_sem.at[far],
            recv_sem=rim_sem.at[j],
            device_id={"seq": lax.rem(core + cores - far, cores)},
            device_id_type=MESH,
        )

    def all_passed(far):
        rims = taps.at[pl.ds(0, direct), pl.ds(block, new)]
        return pltpu.make_async_remote_copy(
            src_ref=rims,
            dst_ref=rims,
            send_sem=pass_sem.at[far],
            recv_sem=rim_sem.at[0],
            device_id={"hist": left},
            device_id_type=MESH,
        )

    def hop(way, owner, i):
        return pltpu.make_async_remote_copy(
            src_ref=send.at[owner, i],
            dst_ref=recv.at[owner + 1 - way, i],
            send_sem=send_sem.at[owner],
            recv_sem=recv_sem.at[owner + 1 - way, i],
            device_id={"hist": right if way == 0 else left},
            device_id_type=MESH,
        )

    def all_sent(owner):
        return pltpu.make_async_remote_copy(
            src_ref=send.at[owner],
            dst_ref=recv.at[owner],
            send_sem=send_sem.at[owner],
            recv_sem=recv_sem.at[owner, 0],
            device_id={"hist": right},
            device_id_type=MESH,
        )

    for copy in small[:3]:
        copy.start()

    def start_loads(i, carry):
        load_taps(i).start()
        load_hist(i).start()
        return carry

    lax.fori_loop(0, min(DEPTH, chunks), start_loads, 0)
    for copy in small[3:]:
        copy.start()

    barrier = pltpu.get_barrier_semaphore()

    @pl.when(jnp.logical_not(last))
    def _():
        pl.semaphore_signal(barrier, inc=1, device_id={"hist": right}, device_id_type=MESH)

    for other in range(1, cores):
        @pl.when(core < other)
        def _():
            pl.semaphore_signal(barrier, inc=1, device_id={"seq": other}, device_id_type=MESH)

    greeted = core + 1 - first.astype(jnp.int32)

    @pl.when(greeted > 0)
    def _():
        pl.semaphore_wait(barrier, greeted)

    def start_rims(i, carry):
        rim_copy(i).start()
        return carry

    @pl.when(jnp.logical_not(first))
    def _():
        pl.semaphore_signal(open_sem.at[0], inc=1, device_id={"hist": left}, device_id_type=MESH)
        lax.fori_loop(0, direct, start_rims, 0)

    for other in range(cores - 1):
        @pl.when(core > other)
        def _():
            pl.semaphore_signal(
                open_sem.at[1], inc=1, device_id={"seq": other}, device_id_type=MESH
            )

    for copy in small:
        copy.wait()
    latest = last.astype(F32)

    def arrive(i):
        @pl.when(i + DEPTH < chunks)
        def _():
            start_loads(i + DEPTH, 0)

        load_taps(i).wait()
        load_hist(i).wait()

    def arrive_rim(i):
        @pl.when(jnp.logical_not(last))
        def _():
            rim_copy(i).wait_recv()

            @pl.when(i < direct)
            def _():
                for far in range(1, cores):
                    rim_pass(i, far).start()

        @pl.when(last)
        def _():
            taps[i, pl.ds(block, new)] = jnp.zeros((new, width), BF16)

    def transform(i, b, slot):
        for q in range(pieces):
            dspec[slot, b, q] = jnp.dot(
                fh[...], hist[i, b, pl.ds(q * piece, piece)], preferred_element_type=F32
            )

    def transform_taps(i, q, slot):
        tspec[slot, q] = jnp.dot(
            ft[...], taps[i, pl.ds(q * piece, piece + new)], preferred_element_type=F32
        )

    def compute(i, slot):
        gains = gain[:, lanes(i)] * latest
        ahead = jnp.minimum(i + 1, chunks - 1)
        for b in range(max(seqs, pieces)):
            if b < seqs:
                transform(ahead, b, 1 - slot)
            if b < pieces:
                transform_taps(ahead, b, 1 - slot)
            if b >= seqs:
                continue
            for r in range(0, bins, 16):
                low, high = pl.ds(2 * r, 16), pl.ds(2 * r + 16, 16)
                real = imag = None
                for q in range(pieces):
                    hc, hs = dspec[slot, b, q, low], dspec[slot, b, q, high]
                    tc, ts = tspec[slot, q, low], tspec[slot, q, high]
                    one, two = tc * hc + ts * hs, ts * hc - tc * hs
                    real = one if q == 0 else real + one
                    imag = two if q == 0 else imag + two
                spec[b, low] = real.astype(BF16)
                spec[b, high] = imag.astype(BF16)
            value = jnp.dot(fi[...], spec[b], preferred_element_type=F32)
            value = value + gains * hist[i, b, pl.ds(block - new, new)].astype(F32)
            for d in range(n):
                part[i, d, b] = value[d * own : (d + 1) * own]

    def pass_on(way, owner, i):
        edge = first if way == 0 else last

        @pl.when(edge)
        def _():
            for b in range(seqs):
                send[owner, i, b] = part[i, owner, b].astype(BF16)

        @pl.when(jnp.logical_not(edge))
        def _():
            hop(way, owner, i).wait_recv()
            for b in range(seqs):
                value = part[i, owner, b] + recv[owner + 1 - way, i, b].astype(F32)
                send[owner, i, b] = value.astype(BF16)

        hop(way, owner, i).start()

    def finish(i):
        @pl.when(jnp.logical_not(first))
        def _():
            hop(0, me, i).wait_recv()
            for b in range(seqs):
                part[i, me, b] += recv[me + 1, i, b].astype(F32)

        @pl.when(jnp.logical_not(last))
        def _():
            hop(1, me, i).wait_recv()
            for b in range(seqs):
                part[i, me, b] += recv[me, i, b].astype(F32)

        for b in range(seqs):
            total[b, :, lanes(i)] = (gate[b, :, lanes(i)].astype(F32) * part[i, me, b]).astype(BF16)

    def guarded(i, action):
        @pl.when(jnp.logical_and(i >= 0, i < chunks))
        def _():
            action(i)

    def turn(way, k):
        gap = RIGHT_GAP if way == 0 else jnp.where(core == 0, LEFT_GAP, OTHER_LEFT_GAP)
        return gap * k + jnp.where(k == n - 2, chunks - gap, 0)

    left_lag = jnp.where(last, 0, LEFT_HOP * ends - 1)
    right_lag = jnp.where(first, 0, RIGHT_HOP * me)
    final = jnp.where(
        jnp.logical_or(first, last),
        jnp.maximum(chunks + jnp.maximum(turn(0, n - 2), turn(1, n - 2)), max(LEFT_HOP, RIGHT_HOP) * n),
        jnp.maximum(left_lag + turn(1, me), right_lag + turn(0, ends)),
    )

    def step(t, slot):
        @pl.when(t + 1 < chunks)
        def _():
            arrive(t + 1)
            arrive_rim(t + 1)

        @pl.when(t < chunks)
        def _():
            compute(t, slot)

        def to_left(k, carry):
            guarded(t - left_lag - turn(1, k), functools.partial(pass_on, 1, k))
            return carry

        def to_right(k, carry):
            guarded(t - right_lag - turn(0, k), functools.partial(pass_on, 0, n - 1 - k))
            return carry

        lax.fori_loop(0, me, to_left, 0)
        lax.fori_loop(0, ends, to_right, 0)
        guarded(t - final, finish)

    def steps(p, carry):
        for slot in range(2):
            step(2 * p + slot, slot)
        return carry

    arrive(0)
    for b in range(seqs):
        transform(0, b, 0)
    for q in range(pieces - 1):
        transform_taps(0, q, 0)

    @pl.when(core < cores - 1)
    def _():
        pl.semaphore_wait(open_sem.at[1], cores - 1 - core)

    arrive_rim(0)
    transform_taps(0, pieces - 1, 0)

    @pl.when(jnp.logical_not(last))
    def _():
        pl.semaphore_wait(open_sem.at[0], 1)

    lax.fori_loop(0, (chunks + final + 1) // 2, steps, 0)

    @pl.when(jnp.logical_not(first))
    def _():
        all_passed(0).wait_send()

    @pl.when(jnp.logical_not(last))
    def _():
        for far in range(1, cores):
            all_passed(far).wait_send()

    def drain(owner, carry):
        @pl.when(owner != me)
        def _():
            all_sent(owner).wait_send()

        return carry

    lax.fori_loop(0, n, drain, 0)


def body(history, filter_taps, skip_gain, gate_values):
    n = lax.axis_size("hist")
    seqs, block, channels = history.shape
    own = gate_values.shape[1]
    new = own * n
    piece = min(2 * new, block)
    width = min(256, channels)
    chunks = channels // width
    length = piece + new
    cores = lax.axis_size("seq")
    hbm = pl.BlockSpec(memory_space=pl.ANY)
    return pl.pallas_call(
        functools.partial(kernel, n, new, piece, width),
        out_shape=pltpu.VMEM(gate_values.shape, BF16),
        in_specs=[hbm] * 7,
        out_specs=pl.BlockSpec(memory_space=pltpu.VMEM),
        scratch_shapes=[
            pltpu.VMEM((length, length), BF16),
            pltpu.VMEM((length, piece), BF16),
            pltpu.VMEM((new, length), BF16),
            pltpu.VMEM((chunks, seqs, block, width), BF16),
            pltpu.VMEM((chunks, block + new, width), BF16),
            pltpu.VMEM((1, channels), F32),
            pltpu.VMEM(gate_values.shape, BF16),
            pltpu.VMEM((2, block // piece, length, width), F32),
            pltpu.VMEM((2, seqs, block // piece, length, width), F32),
            pltpu.VMEM((seqs, length, width), BF16),
            pltpu.VMEM((chunks, n, seqs, own, width), F32),
            pltpu.VMEM((n, chunks, seqs, own, width), BF16),
            pltpu.VMEM((n + 1, chunks, seqs, own, width), BF16),
            pltpu.SemaphoreType.DMA((2, DEPTH + 1)),
            pltpu.SemaphoreType.DMA((5,)),
            pltpu.SemaphoreType.DMA((chunks,)),
            pltpu.SemaphoreType.DMA((cores,)),
            pltpu.SemaphoreType.REGULAR((2,)),
            pltpu.SemaphoreType.DMA((n,)),
            pltpu.SemaphoreType.DMA((n + 1, chunks)),
        ],
        compiler_params=pltpu.CompilerParams(
            collective_id=0, has_side_effects=True, vmem_limit_bytes=60 * 2**20
        ),
    )(*tables(new, piece), history, filter_taps, skip_gain[None, :], gate_values)


def solution(mesh):
    placed = (
        P(("grp", "seq"), "hist", "chan"),
        P(("grp", "hist"), "chan"),
        P(("grp", "chan")),
        P(("grp", "seq"), "hist", "chan"),
    )
    return jax.shard_map(
        body,
        mesh=mesh,
        in_specs=placed,
        out_specs=P(("grp", "seq"), "hist", "chan"),
        check_vma=False,
    )
```
